256 devices in a mesh: graph: 16 (over z, y_lo), row: 16 (over y_hi, x, core).
Axes of the slice: x: 4, y: 4 (y_hi: 2, y_lo: 2; y = y_hi * 2 + y_lo), z: 8, core: 2. Of those that a mesh axis runs over, the one named last changes fastest.
Arguments:
- tiles: bfloat16 [16384, 256, 256], P(('graph', 'row')), parts along dimension 0, may hold values from -0.25 to 0.25
- tile_rows: int32 [16384], P(('graph', 'row')), parts along dimension 0, may hold values from 0 to 15
- tile_cols: int32 [16384], P(('graph', 'row')), parts along dimension 0, may hold values from 0 to 255, as said below
- tile_count: int32 [256], P(('graph', 'row')), parts along dimension 0, may hold values from 8 to 64, as said below
- seeds: float32 [32, 1048576], P(None, ('graph', 'row')), parts along dimension 1, may hold values from -6 to 6
- decay: float32 [32], replicated, may hold values from 0.8 to 1
Outputs:
- scores: float32 [32, 1048576], P(None, ('graph', 'row')), parts along dimension 1
The draws below stay inside these ranges and needn't reach their ends.
There are 16 independent parts, one for each index of `graph`. The reference program is written for one: setup_inputs(seed, part) draws one part's arguments, and reference() takes and returns one part's arrays. A program takes and returns all parts, laid end to end along the dimension named above; an argument that names none is the same for every part. Nothing has to cross between parts.
Inputs may be any that keep to these rules, and one draw needn't show every extreme that they name: `tile_cols`: among the slots of one row panel, the tile columns that fall in the 16 tile rows of any one panel take at most 4 distinct values; in every draw the live slots of some panel take exactly 4 distinct tile columns of some one panel. Only the first tile_count slots of a panel are live; in every draw one panel has all 64 slots live.
All inputs are finite; a program needn't handle non-finite values.
Results may differ from the reference program's by a relative error of at most 0.0027.
Values may be sent and summed in bfloat16 or wider, within the bound.
A program may use at most 64 MiB of HBM per device.

```python
import jax
import jax.numpy as jnp
from jax import lax

TILE = 256
SEEDS = 32
BLK_DEV = 16
TILES_DEV = 64
NEED = 4
ITERS = 3
NBLK = 256
ORDER = 65536
TILES = 1024
N_ROW = 16


def draw_tile_rows(key, part):
    return jax.random.randint(jax.random.fold_in(key, 11), (N_ROW * TILES_DEV,), 0, BLK_DEV).astype(jnp.int32)


def fullest_panel(key):
    return jax.random.randint(jax.random.fold_in(key, 14), (), 0, N_ROW)


def draw_tile_cols(key, part):
    pair_keys = jax.random.split(jax.random.fold_in(key, 21), N_ROW * N_ROW)
    choices = jax.vmap(lambda one: jax.random.permutation(one, BLK_DEV)[:NEED])(pair_keys)
    choices = choices.reshape(N_ROW, N_ROW, NEED).astype(jnp.int32)
    owning_panels = jax.random.randint(jax.random.fold_in(key, 22), (N_ROW, TILES_DEV), 0, N_ROW)
    picks = jax.random.randint(jax.random.fold_in(key, 23), (N_ROW, TILES_DEV), 0, NEED)
    fullest = fullest_panel(key)
    chosen_owner = jax.random.randint(jax.random.fold_in(key, 24), (), 0, N_ROW)
    panels = jnp.arange(N_ROW, dtype=jnp.int32)[:, None]
    slots = jnp.arange(TILES_DEV, dtype=jnp.int32)[None, :]
    forced = (panels == fullest) & (slots < NEED)
    owning_panels = jnp.where(forced, chosen_owner, owning_panels).astype(jnp.int32)
    picks = jnp.where(forced, slots, picks).astype(jnp.int32)
    panel_full = jnp.broadcast_to(panels, (N_ROW, TILES_DEV))
    local = choices[panel_full, owning_panels, picks]
    return (owning_panels * BLK_DEV + local).reshape(N_ROW * TILES_DEV).astype(jnp.int32)


def draw_tile_count(key, part):
    lower = max(TILES_DEV // 8, 1)
    base = jax.random.randint(jax.random.fold_in(key, 13), (N_ROW,), lower, TILES_DEV // 2 + 1)
    fullest = fullest_panel(key)
    panels = jnp.arange(N_ROW, dtype=jnp.int32)
    return jnp.where(panels == fullest, TILES_DEV, base).astype(jnp.int32)


def block_scale(key, extent, pieces, low, largest):
    def one(axis_at, parts):
        draws = jax.random.uniform(jax.random.fold_in(jax.random.fold_in(key, 6), axis_at), (parts,), jnp.float32, low / len(pieces), largest / len(pieces))
        return jnp.repeat(jnp.exp(draws), extent[axis_at] // parts).reshape((-1,) + (1,) * (len(extent) - axis_at - 1))

    gain = one(*pieces[0])
    for cut in pieces[1:]:
        gain = gain * one(*cut)
    return gain


def normal_values(own_key, extent, spread, limit, cuts=(), kind=jnp.bfloat16):
    entries = jax.random.normal(own_key, extent, jnp.float32) * spread
    if len(cuts) > 0:
        entries = block_scale(own_key, extent, cuts, -0.22, 0.18) * entries
    return jnp.clip(entries, min=-limit, max=limit).astype(kind)


def setup_inputs(seed: int = 0, part: int = 0) -> dict:
    splits = jax.random.split(jax.random.key(seed), 7)
    part_splits = jax.random.split(jax.random.fold_in(splits[6], part), 7)
    return {
        "tiles": normal_values(part_splits[0], (TILES, TILE, TILE), (TILE * 2) ** -0.5, 0.25, ((0, 16),)),
        "tile_rows": draw_tile_rows(jax.random.fold_in(jax.random.fold_in(splits[6], part), 71), part),
        "tile_cols": draw_tile_cols(jax.random.fold_in(jax.random.fold_in(splits[6], part), 71), part),
        "tile_count": draw_tile_count(jax.random.fold_in(jax.random.fold_in(splits[6], part), 71), part),
        "seeds": normal_values(part_splits[4], (SEEDS, ORDER), 1.0, 6.0, ((1, 16),), jnp.float32),
        "decay": jnp.clip(jax.random.uniform(splits[5], (SEEDS,), jnp.float32, 0.8, 1.0), 0.8, 1.0),
    }


def reference(tiles, tile_rows, tile_cols, tile_count, seeds, decay):
    slot_index = jnp.arange(N_ROW * TILES_DEV, dtype=jnp.int32)
    panel = slot_index // TILES_DEV
    active_flag = slot_index % TILES_DEV < tile_count[panel]
    target = (panel * BLK_DEV + tile_rows).astype(jnp.int32)
    weight = active_flag.astype(jnp.float32)
    tiles_wide = tiles.astype(jnp.float32)
    iterate = seeds
    for step in range(ITERS):
        rounded = iterate.astype(jnp.bfloat16)
        blocks = rounded.reshape(SEEDS, NBLK, TILE)
        picked = jnp.take(blocks, tile_cols, axis=1).astype(jnp.float32)
        block_products = jnp.einsum('trc,stc->tsr', tiles_wide, picked, precision=lax.Precision.HIGHEST)
        block_products = block_products * weight[:, None, None]
        reduced_sum = jax.ops.segment_sum(block_products, target, num_segments=NBLK)
        reduced_sum = jnp.transpose(reduced_sum, (1, 0, 2)).reshape(SEEDS, NBLK * TILE)
        iterate = decay[:, None] * reduced_sum + seeds
    norm_value = jnp.sqrt(lax.optimization_barrier(jnp.mean(iterate * iterate, axis=1, keepdims=True)) + 1e-06)
    return iterate / norm_value
```

```python
import functools

import jax
import jax.numpy as jnp
from jax import lax
from jax.experimental import pallas as pl
from jax.experimental.pallas import tpu as pltpu
from jax.sharding import PartitionSpec as P

TILE = 256
NEED = 4
ITERS = 3
HALVES = 2
MESH = pl.DeviceIdType.MESH
NEG = [(d // 8) * 8 + ((4 - (d // 2) % 4) % 4) * 2 + d % 2 for d in range(16)]


def hops(d):
    dx = (d // 2) % 4
    return min(dx, 4 - dx) + 2 * (d // 8)


FAR = sorted(range(1, 16), key=lambda d: (-hops(d), d))


def kernel(
    tiles_hbm, rows_ref, cols_ref, count_ref, seeds_hbm, decay_ref,
    out_hbm, norm_ref,
    tiles, tiles_t, seeds, own, sendbuf,
    recv0, recv1, recv2, recv3, recv4, recv5, pref, res,
    meta_out, meta_in, meta_sm, tab, tab_sm, sq_out, sq_in,
    load_sem, tab_sem, self_sem, meta_ssem, meta_rsem, asm_sem,
    ssem, rsem, sq_ssem, sq_rsem, out_sem,
):
    slots = tiles.shape[0]
    n_row = 16
    blk = 16
    recv = [recv0, recv1, recv2, recv3, recv4, recv5]
    phases = ITERS * HALVES
    half = seeds.shape[0] // HALVES
    me = lax.axis_index("row")
    my_y, my_x, my_c = me // 8, lax.rem(me // 2, 4), lax.rem(me, 2)

    def peer(d):
        py = lax.rem(my_y + d // 8, 2)
        px = lax.rem(my_x + (d // 2) % 4, 4)
        pc = lax.rem(my_c + d % 2, 2)
        return {"row": py * 8 + px * 2 + pc}

    def bounded(i, n):
        return jnp.minimum(jnp.maximum(i, 0), n - 1)

    barrier = pltpu.get_barrier_semaphore()
    for d in FAR:
        pl.semaphore_signal(barrier, inc=1, device_id=peer(d), device_id_type=MESH)

    seed_load = pltpu.make_async_copy(seeds_hbm, seeds, load_sem.at[8])
    seed_load.start()
    part = slots // 8
    tile_loads = [
        pltpu.make_async_copy(tiles_hbm.at[pl.ds(i * part, part)], tiles.at[pl.ds(i * part, part)], load_sem.at[i])
        for i in range(8)
    ]
    for copy in tile_loads:
        copy.start()

    f32 = jnp.float32
    i32 = jnp.int32

    def iota(shape, axis):
        return lax.broadcasted_iota(i32, shape, axis)

    def total(hit, v, axis):
        return jnp.sum(jnp.where(hit, v, 0), axis=axis, keepdims=True)

    ncol = n_row * blk
    cols_l = cols_ref[...]
    live_l = iota((1, slots), 1) < count_ref[...]
    key_l = jnp.where(live_l, rows_ref[...], blk)
    sub = iota((slots, slots), 0)
    lane = iota((slots, slots), 1)
    cols_s = total(sub == lane, cols_l, 1)
    key_s = total(sub == lane, key_l, 1)
    before = (key_l == key_s) & (lane < sub)
    pos_s = total((key_l < key_s) | before, 1, 1)
    keep_s = jnp.minimum(total(before, 1, 1), 1)
    place_hot = pos_s == lane

    present_s = jnp.minimum(total((cols_l == iota((ncol, slots), 0)) & live_l, 1, 1), 1)
    c_a = iota((ncol, ncol), 0)
    c_b = iota((ncol, ncol), 1)
    rank_l = total((c_a // blk == c_b // blk) & (c_a < c_b), present_s, 0)
    present_l = total(c_a == c_b, present_s, 0)
    c_l = iota((1, ncol), 1)
    owner = c_l // blk
    slot_l = (
        ((my_y + 2 - owner // 8) % 2) * 8
        + ((my_x + 4 - (owner // 2) % 4) % 4) * 2
        + (my_c + 2 - owner % 2) % 2
    )
    place_l = slot_l * NEED + jnp.minimum(rank_l, NEED - 1)
    place_s = total(cols_s == c_l, place_l, 1)
    mine = (slot_l == iota((16, ncol), 0)) & (present_l > 0)
    wanted = jnp.zeros((16, 128), i32)
    for k in range(NEED):
        pick = total(mine & (rank_l == k), c_l % blk, 1)
        wanted = jnp.where(iota((16, 128), 1) == k, pick, wanted)
    for d in range(16):
        meta_out[d] = wanted[d:d + 1, :]

    slot_id = iota((slots, 1), 0)
    tab[0:1, 0:slots] = total(place_hot, slot_id, 0)
    tab[1:2, 0:slots] = total(place_hot, place_s, 0)
    tab[2:3, 0:slots] = total(place_hot, keep_s, 0)
    upto = total(key_s <= lane, 1, 0)
    tab[3:4, 0:slots] = jnp.maximum(upto - 1, 0)
    tab[4:5, 0:slots] = total(key_s == lane, 1, 0)

    tab_copy = pltpu.make_async_copy(tab, tab_sm, tab_sem)
    tab_copy.start()
    self_copy = pltpu.make_async_copy(meta_out.at[0], meta_sm.at[0], self_sem)
    self_copy.start()

    pl.semaphore_wait(barrier, n_row - 1)

    def request(d):
        return pltpu.make_async_remote_copy(
            src_ref=meta_out.at[d], dst_ref=meta_in.at[d],
            send_sem=meta_ssem.at[d], recv_sem=meta_rsem.at[d],
            device_id=peer(NEG[d]), device_id_type=MESH,
        )

    for d in FAR:
        request(d).start()

    decay_l = decay_ref[...]
    nseed = seeds.shape[0]
    e_sub = lax.broadcasted_iota(i32, (nseed, nseed), 0)
    e_lane = lax.broadcasted_iota(i32, (nseed, nseed), 1)
    decay = jnp.sum(jnp.where(e_sub == e_lane, decay_l, 0.0), axis=1, keepdims=True)
    res[0:nseed, 0:128] = jnp.broadcast_to(decay, (nseed, 128))

    seed_load.wait()
    tab_copy.wait()
    self_copy.wait()

    def exchange(p, d):
        return pltpu.make_async_remote_copy(
            src_ref=sendbuf.at[p, pl.ds(d * NEED, NEED)], dst_ref=recv[p].at[pl.ds(d * NEED, NEED)],
            send_sem=ssem.at[p, d], recv_sem=rsem.at[p, d],
            device_id=peer(d), device_id_type=MESH,
        )

    def fill(p, d):
        for k in range(NEED):
            sendbuf[p, d * NEED + k] = own[p, bounded(meta_sm[d, 0, k], blk)]

    def fill_self(p):
        for k in range(NEED):
            recv[p][k] = own[p, bounded(meta_sm[0, 0, k], blk)]

    for h in range(HALVES):
        for r in range(blk):
            own[h, r] = seeds[h * half:(h + 1) * half, r * TILE:(r + 1) * TILE].astype(jnp.bfloat16)
    near = FAR[::-1]
    for d in near:
        request(d).wait_recv()
        to_sm = pltpu.make_async_copy(meta_in.at[d], meta_sm.at[d], asm_sem.at[d])
        to_sm.start()
    for d in near:
        pltpu.make_async_copy(meta_in.at[d], meta_sm.at[d], asm_sem.at[d]).wait()
    for p in range(HALVES):
        last = None
        for d in FAR:
            fill(p, d)
            if last is not None:
                exchange(p, last).start()
            last = d
        fill_self(p)
        exchange(p, last).start()
    for copy in tile_loads:
        copy.wait()

    def turn(i, _):
        tiles_t[i] = tiles[bounded(tab_sm[0, i], slots)].T
        return 0

    lax.fori_loop(0, slots, turn, 0, unroll=4)
    for d in FAR:
        request(d).wait_send()

    group = 16

    def phase(p):
        h = p % HALVES
        for d in FAR:
            exchange(p, d).wait_recv()

        def tiles_step(g, acc):
            for u in range(group):
                i = g * group + u
                product = jnp.dot(recv[p][bounded(tab_sm[1, i], n_row * NEED)], tiles_t[i], preferred_element_type=f32)
                acc = jnp.where(tab_sm[2, i] > 0, acc, 0.0) + product
                pref[i] = acc
            return acc

        lax.fori_loop(0, slots // group, tiles_step, jnp.zeros((half, TILE), f32))
        rows_h = pl.ds(h * half, half)
        gain = res[rows_h, 0:1]

        def value(r):
            reach = jnp.where(tab_sm[4, r] > 0, pref[bounded(tab_sm[3, r], slots)], 0.0)
            return gain * reach + seeds[rows_h, r * TILE:(r + 1) * TILE]

        if p < phases - HALVES:
            nxt = p + HALVES
            for r in range(blk):
                own[nxt, r] = value(r).astype(jnp.bfloat16)
            last = None
            for d in FAR:
                fill(nxt, d)
                if last is not None:
                    exchange(nxt, last).start()
                last = d
            fill_self(nxt)
            exchange(nxt, last).start()

        else:
            square = jnp.zeros((half, TILE), f32)
            for r in range(blk):
                v = value(r)
                res[rows_h, 128 + r * TILE:128 + (r + 1) * TILE] = v
                square = square + v * v
            energy = jnp.sum(square, axis=1, keepdims=True)
            q_sub = lax.broadcasted_iota(i32, (half, 128), 0)
            q_lane = lax.broadcasted_iota(i32, (half, 128), 1)
            flat = jnp.sum(jnp.where(q_sub == q_lane, energy, 0.0), axis=0, keepdims=True)
            sq_out[h] = flat
            sq_in[h, 0] = flat
            for d in FAR:
                squares(h, d).start()
            pltpu.make_async_copy(
                res.at[rows_h, pl.ds(128, blk * TILE)], out_hbm.at[rows_h, :], out_sem.at[h]
            ).start()

        for d in FAR:
            exchange(p, d).wait_send()

    def squares(h, d):
        return pltpu.make_async_remote_copy(
            src_ref=sq_out.at[h], dst_ref=sq_in.at[h, d],
            send_sem=sq_ssem.at[h, d], recv_sem=sq_rsem.at[h, d],
            device_id=peer(d), device_id_type=MESH,
        )

    for p in range(phases):
        phase(p)
    for h in range(HALVES):
        for d in FAR:
            squares(h, d).wait()
    for h in range(HALVES):
        acc = sq_in[h, 0]
        for d in range(1, 16):
            acc = acc + sq_in[h, d]
        norm_ref[h:h + 1, :] = acc
    for h in range(HALVES):
        pltpu.make_async_copy(
            res.at[pl.ds(h * half, half), pl.ds(128, blk * TILE)],
            out_hbm.at[pl.ds(h * half, half), :], out_sem.at[h],
        ).wait()


def per_device(tiles, tile_rows, tile_cols, tile_count, seeds, decay):
    slots = tiles.shape[0]
    nseed, width = seeds.shape
    blk = width // TILE
    n_row = lax.axis_size("row")
    half = nseed // HALVES
    phases = ITERS * HALVES
    bf16, f32, i32 = jnp.bfloat16, jnp.float32, jnp.int32
    vmem = pl.BlockSpec(memory_space=pltpu.VMEM)
    anywhere = pl.BlockSpec(memory_space=pl.ANY)
    dma = pltpu.SemaphoreType.DMA
    iterate, squares = pl.pallas_call(
        kernel,
        out_shape=(
            jax.ShapeDtypeStruct((nseed, width), f32),
            jax.ShapeDtypeStruct((HALVES, 128), f32),
        ),
        in_specs=[anywhere, vmem, vmem, vmem, anywhere, vmem],
        out_specs=(anywhere, vmem),
        scratch_shapes=[
            pltpu.VMEM((slots, TILE, TILE), bf16),
            pltpu.VMEM((slots, TILE, TILE), bf16),
            pltpu.VMEM((nseed, width), f32),
            pltpu.VMEM((phases, blk, half, TILE), bf16),
            pltpu.VMEM((phases, n_row * NEED, half, TILE), bf16),
            *[pltpu.VMEM((n_row * NEED, half, TILE), bf16) for _ in range(phases)],
            pltpu.VMEM((slots, half, TILE), f32),
            pltpu.VMEM((nseed, 128 + width), f32),
            pltpu.VMEM((16, 1, 128), i32),
            pltpu.VMEM((16, 1, 128), i32),
            pltpu.SMEM((16, 1, 128), i32),
            pltpu.VMEM((8, 128), i32),
            pltpu.SMEM((8, 128), i32),
            pltpu.VMEM((HALVES, 1, 128), f32),
            pltpu.VMEM((HALVES, 16, 1, 128), f32),
            dma((9,)), dma, dma, dma((16,)), dma((16,)), dma((16,)),
            dma((phases, 16)), dma((phases, 16)), dma((HALVES, 16)), dma((HALVES, 16)), dma((HALVES,)),
        ],
        compiler_params=pltpu.CompilerParams(collective_id=0, has_side_effects=True),
        name="katz",
    )(
        tiles, tile_rows.reshape(1, slots), tile_cols.reshape(1, slots),
        tile_count.reshape(1, 1), seeds, decay.reshape(1, nseed),
    )
    total_nodes = n_row * width
    norm_value = jnp.sqrt(squares[:, :half].reshape(nseed) / total_nodes + 1e-06)
    return iterate / norm_value[:, None]


def solution(mesh):
    in_specs = (
        P(("graph", "row"), None, None),
        P(("graph", "row")),
        P(("graph", "row")),
        P(("graph", "row")),
        P(None, ("graph", "row")),
        P(),
    )
    out_specs = P(None, ("graph", "row"))
    return jax.shard_map(
        per_device, mesh=mesh, in_specs=in_specs, out_specs=out_specs, check_vma=False
    )
```

```python
import functools

import jax
import jax.numpy as jnp
from jax import lax
from jax.experimental import pallas as pl
from jax.experimental.pallas import tpu as pltpu
from jax.sharding import PartitionSpec as P

TILE = 256
NEED = 4
ITERS = 3
HALVES = 2
MESH = pl.DeviceIdType.MESH
NEG = [(d // 8) * 8 + ((4 - (d // 2) % 4) % 4) * 2 + d % 2 for d in range(16)]


def hops(d):
    dx = (d // 2) % 4
    return min(dx, 4 - dx) + 2 * (d // 8)


FAR = sorted(range(1, 16), key=lambda d: (-hops(d), d))


def kernel(
    tiles_hbm, rows_hbm, cols_hbm, count_ref, seeds_hbm, decay_hbm,
    out_ref,
    tiles, tiles_t, seeds, own, sendbuf,
    recv0, recv1, recv2, recv3, recv4, recv5, pref, res,
    rows_v, cols_v, decay_v, meta_out, meta_sm, tab, tab_sm, sq_out, sq_in,
    load_sem, tab_sem, self_sem, meta_ssem, meta_rsem,
    ssem, rsem, sq_ssem, sq_rsem,
):
    slots = tiles.shape[0]
    n_row = 16
    blk = 16
    recv = [recv0, recv1, recv2, recv3, recv4, recv5]
    phases = ITERS * HALVES
    half = seeds.shape[0] // HALVES
    me = lax.axis_index("row")
    my_y, my_x, my_c = me // 8, lax.rem(me // 2, 4), lax.rem(me, 2)

    def peer(d):
        py = lax.rem(my_y + d // 8, 2)
        px = lax.rem(my_x + (d // 2) % 4, 4)
        pc = lax.rem(my_c + d % 2, 2)
        return {"row": py * 8 + px * 2 + pc}

    def bounded(i, n):
        return jnp.minimum(jnp.maximum(i, 0), n - 1)

    barrier = pltpu.get_barrier_semaphore()
    for d in FAR:
        pl.semaphore_signal(barrier, inc=1, device_id=peer(d), device_id_type=MESH)

    small_loads = [
        pltpu.make_async_copy(src, dst, load_sem.at[9 + i])
        for i, (src, dst) in enumerate(((cols_hbm, cols_v), (rows_hbm, rows_v), (decay_hbm, decay_v)))
    ]
    for copy in small_loads:
        copy.start()
    seed_load = pltpu.make_async_copy(seeds_hbm, seeds, load_sem.at[8])
    seed_load.start()
    part = slots // 8
    tile_loads = [
        pltpu.make_async_copy(tiles_hbm.at[pl.ds(i * part, part)], tiles.at[pl.ds(i * part, part)], load_sem.at[i])
        for i in range(8)
    ]
    for copy in tile_loads:
        copy.start()

    for copy in small_loads:
        copy.wait()
    f32 = jnp.float32
    i32 = jnp.int32

    def iota(shape, axis):
        return lax.broadcasted_iota(i32, shape, axis)

    def total(hit, v, axis):
        return jnp.sum(jnp.where(hit, v, 0), axis=axis, keepdims=True)

    ncol = n_row * blk
    cols_l = cols_v[...]
    live_l = iota((1, slots), 1) < count_ref[0]
    key_l = jnp.where(live_l, rows_v[...], blk)
    sub = iota((slots, slots), 0)
    lane = iota((slots, slots), 1)
    cols_s = total(sub == lane, cols_l, 1)
    present_s = jnp.minimum(total((cols_l == iota((ncol, slots), 0)) & live_l, 1, 1), 1)
    c_a = iota((ncol, ncol), 0)
    c_b = iota((ncol, ncol), 1)
    rank_l = total(((c_a >> 4) == (c_b >> 4)) & (c_a < c_b), present_s, 0)
    present_l = total(c_a == c_b, present_s, 0)
    c_l = iota((1, ncol), 1)
    owner = c_l >> 4
    slot_l = (
        ((my_y + 2 - (owner >> 3)) & 1) * 8
        + ((my_x + 4 - ((owner >> 1) & 3)) & 3) * 2
        + ((my_c + 2 - owner) & 1)
    )
    place_l = slot_l * NEED + jnp.minimum(rank_l, NEED - 1)
    mine = (slot_l == iota((16, ncol), 0)) & (present_l > 0)
    wanted = jnp.zeros((16, 128), i32)
    for k in range(NEED):
        pick = total(mine & (rank_l == k), c_l & 15, 1)
        wanted = jnp.where(iota((16, 128), 1) == k, pick, wanted)
    for d in range(16):
        meta_out[d] = wanted[d:d + 1, :]

    self_copy = pltpu.make_async_copy(meta_out.at[0], meta_sm.at[0], self_sem)
    self_copy.start()

    pl.semaphore_wait(barrier, n_row - 1)

    def request(d):
        return pltpu.make_async_remote_copy(
            src_ref=meta_out.at[d], dst_ref=meta_sm.at[d],
            send_sem=meta_ssem.at[d], recv_sem=meta_rsem.at[d],
            device_id=peer(NEG[d]), device_id_type=MESH,
        )

    for d in FAR:
        request(d).start()

    key_s = total(sub == lane, key_l, 1)
    before = (key_l == key_s) & (lane < sub)
    pos_s = total((key_l < key_s) | before, 1, 1)
    keep_s = jnp.minimum(total(before, 1, 1), 1)
    place_hot = pos_s == lane

    place_s = total(cols_s == c_l, place_l, 1)
    slot_id = iota((slots, 1), 0)
    tab[0:1, 0:slots] = total(place_hot, slot_id, 0)
    tab[1:2, 0:slots] = total(place_hot, place_s, 0)
    tab[2:3, 0:slots] = total(place_hot, keep_s, 0)
    upto = total(key_s <= lane, 1, 0)
    tab[3:4, 0:slots] = jnp.maximum(upto - 1, 0)
    tab[4:5, 0:slots] = total(key_s == lane, 1, 0)

    tab_copy = pltpu.make_async_copy(tab, tab_sm, tab_sem)
    tab_copy.start()

    decay_l = decay_v[...]
    nseed = seeds.shape[0]
    e_sub = lax.broadcasted_iota(i32, (nseed, nseed), 0)
    e_lane = lax.broadcasted_iota(i32, (nseed, nseed), 1)
    decay = jnp.sum(jnp.where(e_sub == e_lane, decay_l, 0.0), axis=1, keepdims=True)
    res[0:nseed, 0:128] = jnp.broadcast_to(decay, (nseed, 128))

    self_copy.wait()

    def exchange(p, d):
        return pltpu.make_async_remote_copy(
            src_ref=sendbuf.at[p, pl.ds(d * NEED, NEED)], dst_ref=recv[p].at[pl.ds(d * NEED, NEED)],
            send_sem=ssem.at[p, d], recv_sem=rsem.at[p, d],
            device_id=peer(d), device_id_type=MESH,
        )

    def fill(p, d):
        for k in range(NEED):
            sendbuf[p, d * NEED + k] = own[p, bounded(meta_sm[d, 0, k], blk)]

    def fill_self(p):
        for k in range(NEED):
            recv[p][k] = own[p, bounded(meta_sm[0, 0, k], blk)]

    seed_load.wait()
    for h in range(HALVES):
        for r in range(blk):
            own[h, r] = seeds[h * half:(h + 1) * half, r * TILE:(r + 1) * TILE].astype(jnp.bfloat16)
    near = FAR[::-1]
    last = None
    for d in near:
        request(d).wait_recv()
        fill(0, d)
        if last is not None:
            exchange(0, last).start()
        last = d
    fill_self(0)
    exchange(0, last).start()
    last = None
    for d in FAR:
        fill(1, d)
        if last is not None:
            exchange(1, last).start()
        last = d
    fill_self(1)
    exchange(1, last).start()
    tab_copy.wait()
    for copy in tile_loads:
        copy.wait()

    def turn(i, _):
        tiles_t[i] = tiles[bounded(tab_sm[0, i], slots)].T
        return 0

    lax.fori_loop(0, slots, turn, 0, unroll=4)
    for d in FAR:
        request(d).wait_send()

    group = 16

    def phase(p):
        h = p % HALVES
        for d in FAR:
            exchange(p, d).wait_recv()

        def tiles_step(g, acc):
            for u in range(group):
                i = g * group + u
                product = jnp.dot(recv[p][bounded(tab_sm[1, i], n_row * NEED)], tiles_t[i], preferred_element_type=f32)
                acc = jnp.where(tab_sm[2, i] > 0, acc, 0.0) + product
                pref[i] = acc
            return acc

        lax.fori_loop(0, slots // group, tiles_step, jnp.zeros((half, TILE), f32))
        rows_h = pl.ds(h * half, half)
        gain = res[rows_h, 0:1]

        def value(r):
            reach = jnp.where(tab_sm[4, r] > 0, pref[bounded(tab_sm[3, r], slots)], 0.0)
            return gain * reach + seeds[rows_h, r * TILE:(r + 1) * TILE]

        if p < phases - HALVES:
            nxt = p + HALVES
            for r in range(blk):
                own[nxt, r] = value(r).astype(jnp.bfloat16)
            last = None
            for d in FAR:
                fill(nxt, d)
                if last is not None:
                    exchange(nxt, last).start()
                last = d
            fill_self(nxt)
            exchange(nxt, last).start()

        else:
            square = jnp.zeros((half, TILE), f32)
            for r in range(blk):
                v = value(r)
                out_ref[rows_h, r * TILE:(r + 1) * TILE] = v
                square = square + v * v
            energy = jnp.sum(square, axis=1, keepdims=True)
            q_sub = lax.broadcasted_iota(i32, (half, 128), 0)
            q_lane = lax.broadcasted_iota(i32, (half, 128), 1)
            flat = jnp.sum(jnp.where(q_sub == q_lane, energy, 0.0), axis=0, keepdims=True)
            sq_out[h] = flat
            sq_in[h, 0] = flat
            for d in FAR:
                squares(h, d).start()

        for d in FAR:
            exchange(p, d).wait_send()

    def squares(h, d):
        return pltpu.make_async_remote_copy(
            src_ref=sq_out.at[h], dst_ref=sq_in.at[h, d],
            send_sem=sq_ssem.at[h, d], recv_sem=sq_rsem.at[h, d],
            device_id=peer(d), device_id_type=MESH,
        )

    for p in range(phases):
        phase(p)
    for h in range(HALVES):
        for d in FAR:
            squares(h, d).wait()
    for h in range(HALVES):
        acc = sq_in[h, 0]
        for d in range(1, 16):
            acc = acc + sq_in[h, d]
        hit = iota((half, 128), 0) == iota((half, 128), 1)
        mean = jnp.sum(jnp.where(hit, acc, 0.0), axis=1, keepdims=True) / (n_row * blk * TILE)
        scale = 1.0 / jnp.sqrt(mean + 1e-06)
        for r in range(blk):
            at = (slice(h * half, (h + 1) * half), slice(r * TILE, (r + 1) * TILE))
            out_ref[at] = out_ref[at] * scale


def per_device(tiles, tile_rows, tile_cols, tile_count, seeds, decay):
    slots = tiles.shape[0]
    nseed, width = seeds.shape
    blk = width // TILE
    n_row = lax.axis_size("row")
    half = nseed // HALVES
    phases = ITERS * HALVES
    bf16, f32, i32 = jnp.bfloat16, jnp.float32, jnp.int32
    vmem = pl.BlockSpec(memory_space=pltpu.VMEM)
    smem = pl.BlockSpec(memory_space=pltpu.SMEM)
    anywhere = pl.BlockSpec(memory_space=pl.ANY)
    dma = pltpu.SemaphoreType.DMA
    return pl.pallas_call(
        kernel,
        out_shape=jax.ShapeDtypeStruct((nseed, width), f32),
        in_specs=[anywhere, anywhere, anywhere, smem, anywhere, anywhere],
        out_specs=vmem,
        scratch_shapes=[
            pltpu.VMEM((slots, TILE, TILE), bf16),
            pltpu.VMEM((slots, TILE, TILE), bf16),
            pltpu.VMEM((nseed, width), f32),
            pltpu.VMEM((phases, blk, half, TILE), bf16),
            pltpu.VMEM((phases, n_row * NEED, half, TILE), bf16),
            *[pltpu.VMEM((n_row * NEED, half, TILE), bf16) for _ in range(phases)],
            pltpu.VMEM((slots, half, TILE), f32),
            pltpu.VMEM((nseed, 128), f32),
            pltpu.VMEM((1, slots), i32),
            pltpu.VMEM((1, slots), i32),
            pltpu.VMEM((1, nseed), f32),
            pltpu.VMEM((16, 1, 128), i32),
            pltpu.SMEM((16, 1, 128), i32),
            pltpu.VMEM((8, 128), i32),
            pltpu.SMEM((8, 128), i32),
            pltpu.VMEM((HALVES, 1, 128), f32),
            pltpu.VMEM((HALVES, 16, 1, 128), f32),
            dma((12,)), dma, dma, dma((16,)), dma((16,)),
            dma((phases, 16)), dma((phases, 16)), dma((HALVES, 16)), dma((HALVES, 16)),
        ],
        compiler_params=pltpu.CompilerParams(collective_id=0, has_side_effects=True),
        name="katz",
    )(
        tiles, tile_rows.reshape(1, slots), tile_cols.reshape(1, slots),
        tile_count, seeds, decay.reshape(1, nseed),
    )


def solution(mesh):
    in_specs = (
        P(("graph", "row"), None, None),
        P(("graph", "row")),
        P(("graph", "row")),
        P(("graph", "row")),
        P(None, ("graph", "row")),
        P(),
    )
    out_specs = P(None, ("graph", "row"))
    return jax.shard_map(
        per_device, mesh=mesh, in_specs=in_specs, out_specs=out_specs, check_vma=False
    )
```

```python
import functools

import jax
import jax.numpy as jnp
from jax import lax
from jax.experimental import pallas as pl
from jax.experimental.pallas import tpu as pltpu
from jax.sharding import PartitionSpec as P

TILE = 256
NEED = 4
ITERS = 3
HALVES = 2
MESH = pl.DeviceIdType.MESH
NEG = [(d // 8) * 8 + ((4 - (d // 2) % 4) % 4) * 2 + d % 2 for d in range(16)]


def hops(d):
    dx = (d // 2) % 4
    return min(dx, 4 - dx) + 2 * (d // 8)


FAR = sorted(range(1, 16), key=lambda d: (-hops(d), d))
MIXED = [13, 3, 7, 5, 9, 11, 15, 2, 6, 4, 12, 8, 10, 14, 1]


def kernel(
    tiles_hbm, rows_hbm, cols_hbm, count_hbm, seeds_hbm, decay_hbm,
    out_ref,
    tiles, tiles_t, seeds, own, sendbuf,
    recv0, recv1, recv2, recv3, recv4, recv5, pref, res,
    rows_v, cols_v, decay_v, count_s, meta_out, meta_sm, tab, tab_sm, sq_out, sq_in,
    load_sem, tab_sem, self_sem, meta_ssem, meta_rsem,
    ssem, rsem, sq_ssem, sq_rsem,
):
    slots = tiles.shape[0]
    n_row = 16
    blk = 16
    recv = [recv0, recv1, recv2, recv3, recv4, recv5]
    phases = ITERS * HALVES
    half = seeds.shape[0] // HALVES
    me = lax.axis_index("row")
    my_y, my_x, my_c = me // 8, lax.rem(me // 2, 4), lax.rem(me, 2)

    def peer(d):
        py = lax.rem(my_y + d // 8, 2)
        px = lax.rem(my_x + (d // 2) % 4, 4)
        pc = lax.rem(my_c + d % 2, 2)
        return {"row": py * 8 + px * 2 + pc}

    def bounded(i, n):
        return jnp.minimum(jnp.maximum(i, 0), n - 1)

    barrier = pltpu.get_barrier_semaphore()
    for d in FAR:
        pl.semaphore_signal(barrier, inc=1, device_id=peer(d), device_id_type=MESH)

    small_loads = [
        pltpu.make_async_copy(src, dst, load_sem.at[9 + i])
        for i, (src, dst) in enumerate(((cols_hbm, cols_v), (count_hbm, count_s), (rows_hbm, rows_v), (decay_hbm, decay_v)))
    ]
    for copy in small_loads:
        copy.start()
    seed_load = pltpu.make_async_copy(seeds_hbm, seeds, load_sem.at[8])
    seed_load.start()
    part = slots // 8
    tile_loads = [
        pltpu.make_async_copy(tiles_hbm.at[pl.ds(i * part, part)], tiles.at[pl.ds(i * part, part)], load_sem.at[i])
        for i in range(8)
    ]
    for copy in tile_loads:
        copy.start()

    for copy in small_loads:
        copy.wait()
    f32 = jnp.float32
    i32 = jnp.int32

    def iota(shape, axis):
        return lax.broadcasted_iota(i32, shape, axis)

    def total(hit, v, axis):
        return jnp.sum(jnp.where(hit, v, 0), axis=axis, keepdims=True)

    ncol = n_row * blk
    cols_l = cols_v[...]
    live_l = iota((1, slots), 1) < count_s[0]
    key_l = jnp.where(live_l, rows_v[...], blk)
    sub = iota((slots, slots), 0)
    lane = iota((slots, slots), 1)
    cols_s = total(sub == lane, cols_l, 1)
    present_s = jnp.minimum(total((cols_l == iota((ncol, slots), 0)) & live_l, 1, 1), 1)
    c_a = iota((ncol, ncol), 0)
    c_b = iota((ncol, ncol), 1)
    rank_l = total(((c_a >> 4) == (c_b >> 4)) & (c_a < c_b), present_s, 0)
    present_l = total(c_a == c_b, present_s, 0)
    c_l = iota((1, ncol), 1)
    owner = c_l >> 4
    slot_l = (
        ((my_y + 2 - (owner >> 3)) & 1) * 8
        + ((my_x + 4 - ((owner >> 1) & 3)) & 3) * 2
        + ((my_c + 2 - owner) & 1)
    )
    place_l = slot_l * NEED + jnp.minimum(rank_l, NEED - 1)
    mine = (slot_l == iota((16, ncol), 0)) & (present_l > 0)
    wanted = jnp.zeros((16, 128), i32)
    for k in range(NEED):
        pick = total(mine & (rank_l == k), c_l & 15, 1)
        wanted = jnp.where(iota((16, 128), 1) == k, pick, wanted)
    for d in range(16):
        meta_out[d] = wanted[d:d + 1, :]

    self_copy = pltpu.make_async_copy(meta_out.at[0], meta_sm.at[0], self_sem)
    self_copy.start()

    pl.semaphore_wait(barrier, n_row - 1)

    def request(d):
        return pltpu.make_async_remote_copy(
            src_ref=meta_out.at[d], dst_ref=meta_sm.at[d],
            send_sem=meta_ssem.at[d], recv_sem=meta_rsem.at[d],
            device_id=peer(NEG[d]), device_id_type=MESH,
        )

    for d in FAR:
        request(d).start()

    key_s = total(sub == lane, key_l, 1)
    before = (key_l == key_s) & (lane < sub)
    pos_s = total((key_l < key_s) | before, 1, 1)
    keep_s = jnp.minimum(total(before, 1, 1), 1)
    place_hot = pos_s == lane

    place_s = total(cols_s == c_l, place_l, 1)
    slot_id = iota((slots, 1), 0)
    tab[0:1, 0:slots] = total(place_hot, slot_id, 0)
    tab[1:2, 0:slots] = total(place_hot, place_s, 0)
    tab[2:3, 0:slots] = total(place_hot, keep_s, 0)
    upto = total(key_s <= lane, 1, 0)
    tab[3:4, 0:slots] = jnp.maximum(upto - 1, 0)
    tab[4:5, 0:slots] = total(key_s == lane, 1, 0)

    tab_copy = pltpu.make_async_copy(tab, tab_sm, tab_sem)
    tab_copy.start()

    decay_l = decay_v[...]
    nseed = seeds.shape[0]
    e_sub = lax.broadcasted_iota(i32, (nseed, nseed), 0)
    e_lane = lax.broadcasted_iota(i32, (nseed, nseed), 1)
    decay = jnp.sum(jnp.where(e_sub == e_lane, decay_l, 0.0), axis=1, keepdims=True)
    res[0:nseed, 0:128] = jnp.broadcast_to(decay, (nseed, 128))

    self_copy.wait()

    def exchange(p, d):
        return pltpu.make_async_remote_copy(
            src_ref=sendbuf.at[p, pl.ds(d * NEED, NEED)], dst_ref=recv[p].at[pl.ds(d * NEED, NEED)],
            send_sem=ssem.at[p, d], recv_sem=rsem.at[p, d],
            device_id=peer(d), device_id_type=MESH,
        )

    def fill(p, d):
        for k in range(NEED):
            sendbuf[p, d * NEED + k] = own[p, bounded(meta_sm[d, 0, k], blk)]

    def fill_self(p):
        for k in range(NEED):
            recv[p][k] = own[p, bounded(meta_sm[0, 0, k], blk)]

    seed_load.wait()
    for h in range(HALVES):
        for r in range(blk):
            own[h, r] = seeds[h * half:(h + 1) * half, r * TILE:(r + 1) * TILE].astype(jnp.bfloat16)
    near = FAR[::-1]
    last = None
    for d in near:
        request(d).wait_recv()
        fill(0, d)
        if last is not None:
            exchange(0, last).start()
        last = d
    fill_self(0)
    exchange(0, last).start()
    last = None
    for d in MIXED:
        fill(1, d)
        if last is not None:
            exchange(1, last).start()
        last = d
    fill_self(1)
    exchange(1, last).start()
    tab_copy.wait()
    for copy in tile_loads:
        copy.wait()

    def turn(i, _):
        tiles_t[i] = tiles[bounded(tab_sm[0, i], slots)].T
        return 0

    lax.fori_loop(0, slots, turn, 0, unroll=4)
    for d in FAR:
        request(d).wait_send()

    group = 32

    def phase(p):
        h = p % HALVES
        for d in FAR:
            exchange(p, d).wait_recv()

        def tiles_step(g, acc):
            for u in range(group):
                i = g * group + u
                product = jnp.dot(recv[p][bounded(tab_sm[1, i], n_row * NEED)], tiles_t[i], preferred_element_type=f32)
                acc = jnp.where(tab_sm[2, i] > 0, acc, 0.0) + product
                pref[i] = acc
            return acc

        lax.fori_loop(0, slots // group, tiles_step, jnp.zeros((half, TILE), f32))
        rows_h = pl.ds(h * half, half)
        gain = res[rows_h, 0:1]

        def value(r):
            reach = jnp.where(tab_sm[4, r] > 0, pref[bounded(tab_sm[3, r], slots)], 0.0)
            return gain * reach + seeds[rows_h, r * TILE:(r + 1) * TILE]

        if p < phases - HALVES:
            nxt = p + HALVES
            for r in range(blk):
                own[nxt, r] = value(r).astype(jnp.bfloat16)
            last = None
            for d in MIXED:
                fill(nxt, d)
                if last is not None:
                    exchange(nxt, last).start()
                last = d
            fill_self(nxt)
            exchange(nxt, last).start()

        else:
            square = jnp.zeros((half, TILE), f32)
            for r in range(blk):
                v = value(r)
                out_ref[rows_h, r * TILE:(r + 1) * TILE] = v
                square = square + v * v
            energy = jnp.sum(square, axis=1, keepdims=True)
            q_sub = lax.broadcasted_iota(i32, (half, 128), 0)
            q_lane = lax.broadcasted_iota(i32, (half, 128), 1)
            flat = jnp.sum(jnp.where(q_sub == q_lane, energy, 0.0), axis=0, keepdims=True)
            sq_out[h] = flat
            sq_in[h, 0] = flat
            for d in FAR:
                squares(h, d).start()

        for d in FAR:
            exchange(p, d).wait_send()

    def squares(h, d):
        return pltpu.make_async_remote_copy(
            src_ref=sq_out.at[h], dst_ref=sq_in.at[h, d],
            send_sem=sq_ssem.at[h, d], recv_sem=sq_rsem.at[h, d],
            device_id=peer(d), device_id_type=MESH,
        )

    for p in range(phases):
        phase(p)
    for h in range(HALVES):
        for d in FAR:
            squares(h, d).wait_recv()
        acc = sq_in[h, 0]
        for d in range(1, 16):
            acc = acc + sq_in[h, d]
        hit = iota((half, 128), 0) == iota((half, 128), 1)
        mean = jnp.sum(jnp.where(hit, acc, 0.0), axis=1, keepdims=True) / (n_row * blk * TILE)
        scale = 1.0 / jnp.sqrt(mean + 1e-06)
        for r in range(blk):
            at = (slice(h * half, (h + 1) * half), slice(r * TILE, (r + 1) * TILE))
            out_ref[at] = out_ref[at] * scale
    for h in range(HALVES):
        for d in FAR:
            squares(h, d).wait_send()


def per_device(tiles, tile_rows, tile_cols, tile_count, seeds, decay):
    slots = tiles.shape[0]
    nseed, width = seeds.shape
    blk = width // TILE
    n_row = lax.axis_size("row")
    half = nseed // HALVES
    phases = ITERS * HALVES
    bf16, f32, i32 = jnp.bfloat16, jnp.float32, jnp.int32
    vmem = pl.BlockSpec(memory_space=pltpu.VMEM)
    anywhere = pl.BlockSpec(memory_space=pl.ANY)
    dma = pltpu.SemaphoreType.DMA
    return pl.pallas_call(
        kernel,
        out_shape=jax.ShapeDtypeStruct((nseed, width), f32),
        in_specs=[anywhere, anywhere, anywhere, anywhere, anywhere, anywhere],
        out_specs=vmem,
        scratch_shapes=[
            pltpu.VMEM((slots, TILE, TILE), bf16),
            pltpu.VMEM((slots, TILE, TILE), bf16),
            pltpu.VMEM((nseed, width), f32),
            pltpu.VMEM((phases, blk, half, TILE), bf16),
            pltpu.VMEM((phases, n_row * NEED, half, TILE), bf16),
            *[pltpu.VMEM((n_row * NEED, half, TILE), bf16) for _ in range(phases)],
            pltpu.VMEM((slots, half, TILE), f32),
            pltpu.VMEM((nseed, 128), f32),
            pltpu.VMEM((1, slots), i32),
            pltpu.VMEM((1, slots), i32),
            pltpu.VMEM((1, nseed), f32),
            pltpu.SMEM((1,), i32),
            pltpu.VMEM((16, 1, 128), i32),
            pltpu.SMEM((16, 1, 128), i32),
            pltpu.VMEM((8, 128), i32),
            pltpu.SMEM((8, 128), i32),
            pltpu.VMEM((HALVES, 1, 128), f32),
            pltpu.VMEM((HALVES, 16, 1, 128), f32),
            dma((13,)), dma, dma, dma((16,)), dma((16,)),
            dma((phases, 16)), dma((phases, 16)), dma((HALVES, 16)), dma((HALVES, 16)),
        ],
        compiler_params=pltpu.CompilerParams(collective_id=0, has_side_effects=True),
        name="katz",
    )(
        tiles, tile_rows.reshape(1, slots), tile_cols.reshape(1, slots),
        tile_count, seeds, decay.reshape(1, nseed),
    )


def solution(mesh):
    in_specs = (
        P(("graph", "row"), None, None),
        P(("graph", "row")),
        P(("graph", "row")),
        P(("graph", "row")),
        P(None, ("graph", "row")),
        P(),
    )
    out_specs = P(None, ("graph", "row"))
    return jax.shard_map(
        per_device, mesh=mesh, in_specs=in_specs, out_specs=out_specs, check_vma=False
    )
```

```python
import functools

import jax
import jax.numpy as jnp
from jax import lax
from jax.experimental import pallas as pl
from jax.experimental.pallas import tpu as pltpu
from jax.sharding import PartitionSpec as P

TILE = 256
NEED = 4
ITERS = 3
HALVES = 2
MESH = pl.DeviceIdType.MESH
NEG = [(d // 8) * 8 + ((4 - (d // 2) % 4) % 4) * 2 + d % 2 for d in range(16)]


def hops(d):
    dx = (d // 2) % 4
    return min(dx, 4 - dx) + 2 * (d // 8)


FAR = sorted(range(1, 16), key=lambda d: (-hops(d), d))
MIXED = [13, 3, 7, 5, 9, 11, 15, 2, 6, 4, 12, 8, 10, 14, 1]


def kernel(
    tiles_hbm, rows_ref, cols_ref, count_ref, seeds_hbm, decay_ref,
    out_ref,
    tiles, tiles_t, seeds, own, sendbuf,
    recv0, recv1, recv2, recv3, recv4, recv5, pref, res,
    meta_out, meta_sm, tab, tab_sm, sq_out, sq_in,
    load_sem, tab_sem, self_sem, meta_ssem, meta_rsem,
    ssem, rsem, sq_ssem, sq_rsem,
):
    slots = tiles.shape[0]
    n_row = 16
    blk = 16
    recv = [recv0, recv1, recv2, recv3, recv4, recv5]
    phases = ITERS * HALVES
    half = seeds.shape[0] // HALVES
    me = lax.axis_index("row")
    my_y, my_x, my_c = me // 8, lax.rem(me // 2, 4), lax.rem(me, 2)

    def peer(d):
        py = lax.rem(my_y + d // 8, 2)
        px = lax.rem(my_x + (d // 2) % 4, 4)
        pc = lax.rem(my_c + d % 2, 2)
        return {"row": py * 8 + px * 2 + pc}

    def bounded(i, n):
        return jnp.minimum(jnp.maximum(i, 0), n - 1)

    barrier = pltpu.get_barrier_semaphore()
    for d in FAR:
        pl.semaphore_signal(barrier, inc=1, device_id=peer(d), device_id_type=MESH)

    seed_load = pltpu.make_async_copy(seeds_hbm, seeds, load_sem.at[8])
    seed_load.start()
    part = slots // 8
    tile_loads = [
        pltpu.make_async_copy(tiles_hbm.at[pl.ds(i * part, part)], tiles.at[pl.ds(i * part, part)], load_sem.at[i])
        for i in range(8)
    ]
    for copy in tile_loads:
        copy.start()

    f32 = jnp.float32
    i32 = jnp.int32

    def iota(shape, axis):
        return lax.broadcasted_iota(i32, shape, axis)

    def total(hit, v, axis):
        return jnp.sum(jnp.where(hit, v, 0), axis=axis, keepdims=True)

    ncol = n_row * blk
    cols_l = cols_ref[...]
    live_l = iota((1, slots), 1) < count_ref[0]
    key_l = jnp.where(live_l, rows_ref[...], blk)
    sub = iota((slots, slots), 0)
    lane = iota((slots, slots), 1)
    cols_s = total(sub == lane, cols_l, 1)
    present_s = jnp.minimum(total((cols_l == iota((ncol, slots), 0)) & live_l, 1, 1), 1)
    c_a = iota((ncol, ncol), 0)
    c_b = iota((ncol, ncol), 1)
    rank_l = total(((c_a >> 4) == (c_b >> 4)) & (c_a < c_b), present_s, 0)
    present_l = total(c_a == c_b, present_s, 0)
    c_l = iota((1, ncol), 1)
    owner = c_l >> 4
    slot_l = (
        ((my_y + 2 - (owner >> 3)) & 1) * 8
        + ((my_x + 4 - ((owner >> 1) & 3)) & 3) * 2
        + ((my_c + 2 - owner) & 1)
    )
    place_l = slot_l * NEED + jnp.minimum(rank_l, NEED - 1)
    mine = (slot_l == iota((16, ncol), 0)) & (present_l > 0)
    wanted = jnp.zeros((16, 128), i32)
    for k in range(NEED):
        pick = total(mine & (rank_l == k), c_l & 15, 1)
        wanted = jnp.where(iota((16, 128), 1) == k, pick, wanted)
    for d in range(16):
        meta_out[d] = wanted[d:d + 1, :]

    self_copy = pltpu.make_async_copy(meta_out.at[0], meta_sm.at[0], self_sem)
    self_copy.start()

    pl.semaphore_wait(barrier, n_row - 1)

    def request(d):
        return pltpu.make_async_remote_copy(
            src_ref=meta_out.at[d], dst_ref=meta_sm.at[d],
            send_sem=meta_ssem.at[d], recv_sem=meta_rsem.at[d],
            device_id=peer(NEG[d]), device_id_type=MESH,
        )

    for d in FAR:
        request(d).start()

    key_s = total(sub == lane, key_l, 1)
    before = (key_l == key_s) & (lane < sub)
    pos_s = total((key_l < key_s) | before, 1, 1)
    keep_s = jnp.minimum(total(before, 1, 1), 1)
    place_hot = pos_s == lane

    place_s = total(cols_s == c_l, place_l, 1)
    slot_id = iota((slots, 1), 0)
    tab[0:1, 0:slots] = total(place_hot, slot_id, 0)
    tab[1:2, 0:slots] = total(place_hot, place_s, 0)
    tab[2:3, 0:slots] = total(place_hot, keep_s, 0)
    upto = total(key_s <= lane, 1, 0)
    tab[3:4, 0:slots] = jnp.maximum(upto - 1, 0)
    tab[4:5, 0:slots] = total(key_s == lane, 1, 0)

    tab_copy = pltpu.make_async_copy(tab, tab_sm, tab_sem)
    tab_copy.start()

    decay_l = decay_ref[...]
    nseed = seeds.shape[0]
    e_sub = lax.broadcasted_iota(i32, (nseed, nseed), 0)
    e_lane = lax.broadcasted_iota(i32, (nseed, nseed), 1)
    decay = jnp.sum(jnp.where(e_sub == e_lane, decay_l, 0.0), axis=1, keepdims=True)
    res[0:nseed, 0:128] = jnp.broadcast_to(decay, (nseed, 128))

    self_copy.wait()

    def exchange(p, d):
        return pltpu.make_async_remote_copy(
            src_ref=sendbuf.at[p, pl.ds(d * NEED, NEED)], dst_ref=recv[p].at[pl.ds(d * NEED, NEED)],
            send_sem=ssem.at[p, d], recv_sem=rsem.at[p, d],
            device_id=peer(d), device_id_type=MESH,
        )

    def fill(p, d):
        for k in range(NEED):
            sendbuf[p, d * NEED + k] = own[p, bounded(meta_sm[d, 0, k], blk)]

    def fill_self(p):
        for k in range(NEED):
            recv[p][k] = own[p, bounded(meta_sm[0, 0, k], blk)]

    seed_load.wait()
    for h in range(HALVES):
        for r in range(blk):
            own[h, r] = seeds[h * half:(h + 1) * half, r * TILE:(r + 1) * TILE].astype(jnp.bfloat16)
    near = FAR[::-1]
    last = None
    for d in near:
        request(d).wait_recv()
        fill(0, d)
        if last is not None:
            exchange(0, last).start()
        last = d
    fill_self(0)
    exchange(0, last).start()
    last = None
    for d in MIXED:
        fill(1, d)
        if last is not None:
            exchange(1, last).start()
        last = d
    fill_self(1)
    exchange(1, last).start()
    tab_copy.wait()
    for copy in tile_loads:
        copy.wait()

    def turn(i, _):
        tiles_t[i] = tiles[bounded(tab_sm[0, i], slots)].T
        return 0

    lax.fori_loop(0, slots, turn, 0, unroll=4)
    for d in FAR:
        request(d).wait_send()

    group = 64

    def phase(p):
        h = p % HALVES
        for d in FAR:
            exchange(p, d).wait_recv()

        def tiles_step(g, acc):
            for u in range(group):
                i = g * group + u
                product = jnp.dot(recv[p][bounded(tab_sm[1, i], n_row * NEED)], tiles_t[i], preferred_element_type=f32)
                acc = jnp.where(tab_sm[2, i] > 0, acc, 0.0) + product
                pref[i] = acc
            return acc

        lax.fori_loop(0, slots // group, tiles_step, jnp.zeros((half, TILE), f32))
        rows_h = pl.ds(h * half, half)
        gain = res[rows_h, 0:1]

        def value(r):
            reach = jnp.where(tab_sm[4, r] > 0, pref[bounded(tab_sm[3, r], slots)], 0.0)
            return gain * reach + seeds[rows_h, r * TILE:(r + 1) * TILE]

        if p < phases - HALVES:
            nxt = p + HALVES
            for r in range(blk):
                own[nxt, r] = value(r).astype(jnp.bfloat16)
            last = None
            for d in MIXED:
                fill(nxt, d)
                if last is not None:
                    exchange(nxt, last).start()
                last = d
            fill_self(nxt)
            exchange(nxt, last).start()

        else:
            square = jnp.zeros((half, TILE), f32)
            for r in range(blk):
                v = value(r)
                out_ref[rows_h, r * TILE:(r + 1) * TILE] = v
                square = square + v * v
            energy = jnp.sum(square, axis=1, keepdims=True)
            q_sub = lax.broadcasted_iota(i32, (half, 128), 0)
            q_lane = lax.broadcasted_iota(i32, (half, 128), 1)
            flat = jnp.sum(jnp.where(q_sub == q_lane, energy, 0.0), axis=0, keepdims=True)
            sq_out[h] = flat
            sq_in[h, 0] = flat
            for d in FAR:
                squares(h, d).start()

        for d in FAR:
            exchange(p, d).wait_send()

    def squares(h, d):
        return pltpu.make_async_remote_copy(
            src_ref=sq_out.at[h], dst_ref=sq_in.at[h, d],
            send_sem=sq_ssem.at[h, d], recv_sem=sq_rsem.at[h, d],
            device_id=peer(d), device_id_type=MESH,
        )

    for p in range(phases):
        phase(p)
    for h in range(HALVES):
        for d in FAR:
            squares(h, d).wait_recv()
        acc = sq_in[h, 0]
        for d in range(1, 16):
            acc = acc + sq_in[h, d]
        hit = iota((half, 128), 0) == iota((half, 128), 1)
        mean = jnp.sum(jnp.where(hit, acc, 0.0), axis=1, keepdims=True) / (n_row * blk * TILE)
        scale = 1.0 / jnp.sqrt(mean + 1e-06)
        for r in range(blk):
            at = (slice(h * half, (h + 1) * half), slice(r * TILE, (r + 1) * TILE))
            out_ref[at] = out_ref[at] * scale
    for h in range(HALVES):
        for d in FAR:
            squares(h, d).wait_send()


def per_device(tiles, tile_rows, tile_cols, tile_count, seeds, decay):
    slots = tiles.shape[0]
    nseed, width = seeds.shape
    blk = width // TILE
    n_row = lax.axis_size("row")
    half = nseed // HALVES
    phases = ITERS * HALVES
    bf16, f32, i32 = jnp.bfloat16, jnp.float32, jnp.int32
    vmem = pl.BlockSpec(memory_space=pltpu.VMEM)
    smem = pl.BlockSpec(memory_space=pltpu.SMEM)
    outside = pl.BlockSpec(memory_space=pltpu.HBM)
    dma = pltpu.SemaphoreType.DMA
    return pl.pallas_call(
        kernel,
        out_shape=jax.ShapeDtypeStruct((nseed, width), f32),
        in_specs=[outside, vmem, vmem, smem, outside, vmem],
        out_specs=vmem,
        scratch_shapes=[
            pltpu.VMEM((slots, TILE, TILE), bf16),
            pltpu.VMEM((slots, TILE, TILE), bf16),
            pltpu.VMEM((nseed, width), f32),
            pltpu.VMEM((phases, blk, half, TILE), bf16),
            pltpu.VMEM((phases, n_row * NEED, half, TILE), bf16),
            *[pltpu.VMEM((n_row * NEED, half, TILE), bf16) for _ in range(phases)],
            pltpu.VMEM((slots, half, TILE), f32),
            pltpu.VMEM((nseed, 128), f32),
            pltpu.VMEM((16, 1, 128), i32),
            pltpu.SMEM((16, 1, 128), i32),
            pltpu.VMEM((8, 128), i32),
            pltpu.SMEM((8, 128), i32),
            pltpu.VMEM((HALVES, 1, 128), f32),
            pltpu.VMEM((HALVES, 16, 1, 128), f32),
            dma((9,)), dma, dma, dma((16,)), dma((16,)),
            dma((phases, 16)), dma((phases, 16)), dma((HALVES, 16)), dma((HALVES, 16)),
        ],
        compiler_params=pltpu.CompilerParams(
            collective_id=0, has_side_effects=True, vmem_limit_bytes=53 * 2**20
        ),
        name="katz",
    )(
        tiles, tile_rows.reshape(1, slots), tile_cols.reshape(1, slots),
        tile_count, seeds, decay.reshape(1, nseed),
    )


def solution(mesh):
    in_specs = (
        P(("graph", "row"), None, None),
        P(("graph", "row")),
        P(("graph", "row")),
        P(("graph", "row")),
        P(None, ("graph", "row")),
        P(),
    )
    out_specs = P(None, ("graph", "row"))
    return jax.shard_map(
        per_device, mesh=mesh, in_specs=in_specs, out_specs=out_specs, check_vma=False
    )
```
